32 devices in a mesh: sp: 8 (over z, y), tp: 4 (over x, core).
Axes of the slice: x: 2, y: 2, z: 4, core: 2. Of those that a mesh axis runs over, the one named last changes fastest.
Arguments:
- decay_rate: float32 [1, 4096, 4096], P(None, 'sp', 'tp'), may hold values from 0.2 to 2
- drive_in: bfloat16 [1, 4096, 4096], P(None, 'sp', 'tp'), may hold values from -6 to 6
- gate_in: bfloat16 [1, 4096, 4096], P(None, 'sp', 'tp'), may hold values from -6 to 6
- norm_gain: float32 [4096], P('tp'), may hold values from 0.25 to 1.75
Outputs:
- filtered: bfloat16 [1, 4096, 4096], P(None, 'sp', 'tp')
The draws below stay inside these ranges and needn't reach their ends.
All inputs are finite; a program needn't handle non-finite values.
Results may differ from the reference program's by a relative error of at most 0.001.
Values sent between devices are 32-bit elements; how exact they have to be, the bound alone decides.
A program may use at most 64 MiB of HBM per device.

```python
import jax
import jax.numpy as jnp
from jax import lax

BATCH = 1
CHANNELS = 4096
LENGTH = 4096


def block_levels(key, extent, cuts, smallest, largest):
    def one(dim, shards_of):
        steps = jax.random.uniform(jax.random.fold_in(jax.random.fold_in(key, 6), dim), (shards_of,), jnp.float32, smallest / len(cuts), largest / len(cuts))
        return jnp.repeat(jnp.exp(steps), extent[dim] // shards_of).reshape((-1,) + (1,) * (len(extent) - dim - 1))

    loudness = one(*cuts[0])
    for cut in cuts[1:]:
        loudness = loudness * one(*cut)
    return loudness


def scatter_about(own_key, shape, width, reach, shards=(), held_as=jnp.bfloat16):
    entries = jax.random.normal(own_key, shape, jnp.float32) * width
    if len(shards) > 0:
        entries = block_levels(own_key, shape, shards, -0.22, 0.18) * entries
    return jnp.clip(entries, min=-reach, max=reach).astype(held_as)


def setup_inputs(seed: int = 0) -> dict:
    key_list = jax.random.split(jax.random.key(seed), 5)
    decay_rate = jnp.clip(0.2 + 1.8 * jax.random.uniform(key_list[0], (BATCH, LENGTH, CHANNELS), jnp.float32) ** block_levels(key_list[0], (BATCH, LENGTH, CHANNELS), ((1, 8), (2, 4)), -0.2, 0.2), 0.2, 2.0)
    drive_in = scatter_about(key_list[1], (BATCH, LENGTH, CHANNELS), 1.0, 6.0, ((1, 8), (2, 4)))
    gate_in = scatter_about(key_list[2], (BATCH, LENGTH, CHANNELS), 1.0, 6.0, ((1, 8), (2, 4)))
    norm_gain = jnp.clip(1.0 + 0.15 * jax.random.normal(key_list[3], (CHANNELS,), jnp.float32), 0.25, 1.75)
    return {"decay_rate": decay_rate, "drive_in": drive_in, "gate_in": gate_in, "norm_gain": norm_gain}


def join_pair(earlier, later):
    return (earlier[0] * later[0], later[0] * earlier[1] + later[1])

def reference(decay_rate, drive_in, gate_in, norm_gain):
    keep = jnp.exp(-decay_rate / LENGTH)
    push = drive_in.astype(jnp.float32) * LENGTH ** (-0.5)
    forward = lax.associative_scan(join_pair, (keep, push), axis=1)[1]
    backward = lax.associative_scan(join_pair, (keep, push), axis=1, reverse=True)[1]
    states = forward + backward
    gated = states * jax.nn.sigmoid(gate_in.astype(jnp.float32))
    power = lax.optimization_barrier(jnp.mean(gated * gated, axis=-1, keepdims=True))
    filtered = (gated * lax.rsqrt(power + 1e-06) * norm_gain).astype(jnp.bfloat16)
    return filtered
```

```python
import functools

import jax
import jax.numpy as jnp
from jax import lax
from jax.experimental import pallas as pl
from jax.experimental.pallas import tpu as pltpu
from jax.sharding import PartitionSpec as P

LANES = 128
SUB = 8
LOG2E = 1.4426950408889634
MESH = pl.DeviceIdType.MESH


def unrolled(count, by, step, carry):
    by = next(size for size in range(min(by, count), 0, -1) if count % size == 0)

    def block(outer, carry):
        for inner in range(by):
            carry = step(outer * by + inner, carry)
        return carry

    return lax.fori_loop(0, count // by, block, carry)


def kernel(
    nsp, ntp, decay, drive, gate, gain, out,
    decay_v, drive_v, gate_v, keep_s, push_s, sig_s, fwd_s, pre_s, suf_s, gated_s,
    inv_s, edge_s, totals, powers, in_sem, tsend, trecv, psend, precv,
):
    rows, channels = decay.shape
    tiles = channels // LANES
    steps = rows // SUB
    length = rows * nsp
    me, mine = lax.axis_index("sp"), lax.axis_index("tp")

    copies = []
    for kind, (source, held) in enumerate(((decay, decay_v), (drive, drive_v), (gate, gate_v))):
        copies.append([
            pltpu.make_async_copy(
                source.at[:, pl.ds(j * LANES, LANES)], held.at[j], in_sem.at[kind, j]
            )
            for j in range(tiles)
        ])
    for j in range(tiles):
        copies[0][j].start()
        copies[1][j].start()
    for j in range(tiles):
        copies[2][j].start()

    barrier = pltpu.get_barrier_semaphore()
    for d in range(1, nsp):
        pl.semaphore_signal(barrier, inc=1, device_id={"sp": lax.rem(me + d, nsp)}, device_id_type=MESH)
    for d in range(1, ntp):
        pl.semaphore_signal(barrier, inc=1, device_id={"tp": lax.rem(mine + d, ntp)}, device_id_type=MESH)

    row = lax.broadcasted_iota(jnp.int32, (SUB, LANES), 0)
    zero = jnp.zeros((SUB, LANES), jnp.float32)
    one = jnp.ones((SUB, LANES), jnp.float32)

    def at(k):
        return pl.ds(k, SUB, stride=steps)

    def packed(k):
        return pl.ds(pl.multiple_of(k * SUB, SUB), SUB)

    group = min(4, tiles)
    for first in range(0, tiles, group):
        members = range(first, min(first + group, tiles))
        for j in members:
            copies[0][j].wait()
            copies[1][j].wait()
            push_s[j] = drive_v[j].astype(jnp.float32)

        def ahead(k, carry):
            after = []
            for j, (prod, fwd, bwd) in zip(members, carry):
                keep = jnp.exp2(decay_v[j, at(k), :] * (-LOG2E / length))
                push = push_s[j, at(k), :]
                bwd = bwd + prod * push
                prod = prod * keep
                fwd = keep * fwd + push
                keep_s[j, packed(k), :] = keep
                fwd_s[j, packed(k), :] = fwd
                pre_s[j, packed(k), :] = prod
                after.append((prod, fwd, bwd))
            return tuple(after)

        ends = unrolled(steps, 8, ahead, tuple((one, zero, zero) for _ in members))
        for j, (prod, fwd, bwd) in zip(members, ends):
            whole, span = prod, prod
            for s in (1, 2, 4):
                keeps = row >= s
                fwd = fwd + whole * jnp.where(keeps, pltpu.roll(fwd, s, 0), 0.0)
                whole = whole * jnp.where(keeps, pltpu.roll(whole, s, 0), 1.0)
                keeps = row < SUB - s
                bwd = bwd + span * jnp.where(keeps, pltpu.roll(bwd, SUB - s, 0), 0.0)
                span = span * jnp.where(keeps, pltpu.roll(span, SUB - s, 0), 1.0)
            totals[me, 0, pl.ds(j, 1), :] = bwd[:1]
            totals[me, 1, pl.ds(j, 1), :] = whole[SUB - 1 :]
            totals[me, 2, pl.ds(j, 1), :] = fwd[SUB - 1 :]
            edge_s[0, j] = jnp.where(row >= 1, pltpu.roll(whole, 1, 0), 1.0)
            edge_s[1, j] = jnp.where(row >= 1, pltpu.roll(fwd, 1, 0), 0.0)
            edge_s[2, j] = jnp.where(row < SUB - 1, pltpu.roll(span, SUB - 1, 0), 1.0)
            edge_s[3, j] = jnp.where(row < SUB - 1, pltpu.roll(bwd, SUB - 1, 0), 0.0)

    pl.semaphore_wait(barrier, nsp + ntp - 2)

    sends = []
    for d in range(1, nsp):
        part = pl.ds(1 - (me + d) // nsp, 2)
        sends.append(pltpu.make_async_remote_copy(
            src_ref=totals.at[me, part],
            dst_ref=totals.at[me, part],
            send_sem=tsend.at[d],
            recv_sem=trecv.at[d],
            device_id={"sp": lax.rem(me + d, nsp)},
            device_id_type=MESH,
        ))
    for copy in sends:
        copy.start()

    for j in range(tiles):
        copies[2][j].wait()

        def squash(k, carry):
            here = pl.ds(pl.multiple_of(k * 2 * SUB, 2 * SUB), 2 * SUB)
            value = gate_v[j, here, :].astype(jnp.float32)
            sig_s[j, here, :] = 1.0 / (1.0 + jnp.exp2(value * -LOG2E))
            return carry

        unrolled(rows // (2 * SUB), 8, squash, 0)

    for first in range(0, tiles, group):
        members = range(first, min(first + group, tiles))

        def astern(i, carry):
            k = steps - 1 - i
            after = []
            for j, (prod, bwd) in zip(members, carry):
                keep = keep_s[j, packed(k), :]
                bwd = keep * bwd + push_s[j, at(k), :]
                prod = keep * prod
                sig = sig_s[j, at(k), :]
                fwd_s[j, packed(k), :] = (fwd_s[j, packed(k), :] + bwd) * sig
                pre_s[j, packed(k), :] = pre_s[j, packed(k), :] * sig
                suf_s[j, packed(k), :] = prod * sig
                after.append((prod, bwd))
            return tuple(after)

        unrolled(steps, 8, astern, tuple((one, zero) for _ in members))

    for copy in sends:
        copy.wait()

    enter_f = jnp.zeros((tiles, LANES), jnp.float32)
    enter_b = jnp.zeros((tiles, LANES), jnp.float32)
    for s in range(nsp - 1):
        enter_f = jnp.where(s < me, totals[s, 1] * enter_f + totals[s, 2], enter_f)
        e = nsp - 1 - s
        enter_b = jnp.where(e > me, totals[e, 1] * enter_b + totals[e, 0], enter_b)
    start_f = [edge_s[0, j] * enter_f[j : j + 1] + edge_s[1, j] for j in range(tiles)]
    start_b = [edge_s[2, j] * enter_b[j : j + 1] + edge_s[3, j] for j in range(tiles)]

    width = powers.shape[-1]
    lane = lax.broadcasted_iota(jnp.int32, (SUB, width), 1)

    def finish(k, sums):
        squares = zero
        for j in range(tiles):
            gated = (
                fwd_s[j, packed(k), :]
                + pre_s[j, packed(k), :] * start_f[j]
                + suf_s[j, packed(k), :] * start_b[j]
            )
            gated_s[j, at(k), :] = gated
            squares = squares + gated * gated
        return jnp.where(lane == k, jnp.sum(squares, axis=1, keepdims=True), sums)

    powers[mine] = unrolled(steps, 8, finish, jnp.zeros((SUB, width), jnp.float32))

    sends = []
    for d in range(1, ntp):
        sends.append(pltpu.make_async_remote_copy(
            src_ref=powers.at[mine],
            dst_ref=powers.at[mine],
            send_sem=psend.at[d],
            recv_sem=precv.at[d],
            device_id={"tp": lax.rem(mine + d, ntp)},
            device_id_type=MESH,
        ))
    for copy in sends:
        copy.start()
    for copy in sends:
        copy.wait()

    power = powers[0]
    for s in range(1, ntp):
        power = power + powers[s]
    power = power * (1.0 / (length * channels * ntp))
    inverse = lax.rsqrt(power + 1e-06) * length ** (-0.5)
    for k in range(steps):
        inv_s[at(k), :] = jnp.broadcast_to(inverse[:, k : k + 1], (SUB, LANES))

    gains = [gain[j : j + 1, :] for j in range(tiles)]

    def emit(k, carry):
        here = pl.ds(pl.multiple_of(k * 2 * SUB, 2 * SUB), 2 * SUB)
        scale = inv_s[here, :]
        for j in range(tiles):
            out[here, pl.ds(j * LANES, LANES)] = (
                gated_s[j, here, :] * scale * gains[j]
            ).astype(jnp.bfloat16)
        return carry

    unrolled(rows // (2 * SUB), 4, emit, 0)


def body(nsp, ntp, decay_rate, drive_in, gate_in, norm_gain):
    batch, rows, channels = decay_rate.shape
    tiles = channels // LANES
    steps = rows // SUB
    width = -(-steps // LANES) * LANES
    plane = pltpu.VMEM((tiles, rows, LANES), jnp.float32)
    half = pltpu.VMEM((tiles, rows, LANES), jnp.bfloat16)
    anywhere = pl.BlockSpec(memory_space=pl.ANY)
    vmem = pl.BlockSpec(memory_space=pltpu.VMEM)
    result = pl.pallas_call(
        functools.partial(kernel, nsp, ntp),
        out_shape=jax.ShapeDtypeStruct((rows, channels), jnp.bfloat16),
        in_specs=[anywhere, anywhere, anywhere, vmem],
        out_specs=vmem,
        scratch_shapes=[
            plane, half, half, plane, plane, plane, plane, plane, plane, plane,
            pltpu.VMEM((rows, LANES), jnp.float32),
            pltpu.VMEM((4, tiles, SUB, LANES), jnp.float32),
            pltpu.VMEM((nsp, 3, tiles, LANES), jnp.float32),
            pltpu.VMEM((ntp, SUB, width), jnp.float32),
            pltpu.SemaphoreType.DMA((3, tiles)),
            pltpu.SemaphoreType.DMA((nsp,)),
            pltpu.SemaphoreType.DMA((nsp,)),
            pltpu.SemaphoreType.DMA((ntp,)),
            pltpu.SemaphoreType.DMA((ntp,)),
        ],
        compiler_params=pltpu.CompilerParams(collective_id=0, has_side_effects=True),
    )(
        decay_rate.reshape(rows, channels),
        drive_in.reshape(rows, channels),
        gate_in.reshape(rows, channels),
        norm_gain.reshape(tiles, LANES),
    )
    return result.reshape(batch, rows, channels)


def solution(mesh):
    in_specs = (P(None, "sp", "tp"), P(None, "sp", "tp"), P(None, "sp", "tp"), P("tp"))
    out_specs = P(None, "sp", "tp")
    local = functools.partial(body, mesh.shape["sp"], mesh.shape["tp"])
    return jax.shard_map(local, mesh=mesh, in_specs=in_specs, out_specs=out_specs, check_vma=False)
```

```python
import functools

import jax
import jax.numpy as jnp
from jax import lax
from jax.experimental import pallas as pl
from jax.experimental.pallas import tpu as pltpu
from jax.sharding import PartitionSpec as P

LANES = 128
SUB = 8
LOG2E = 1.4426950408889634
MESH = pl.DeviceIdType.MESH


def unrolled(count, by, step, carry):
    by = next(size for size in range(min(by, count), 0, -1) if count % size == 0)

    def block(outer, carry):
        for inner in range(by):
            carry = step(outer * by + inner, carry)
        return carry

    return lax.fori_loop(0, count // by, block, carry)


def spaced(steps):
    return steps + next(more for more in range(4, 40, 4) if (steps + more) % 8 == 4)


def kernel(
    nsp, ntp, decay, drive, gate, gain, out,
    decay_v, drive_v, gate_v, decay_s, push_s, sig_s, fwd_s, pre_s, suf_s, gated_s,
    inv_s, edge_s, totals, powers, gain_v, gain_sem, in_sem, tsend, trecv, psend, precv,
):
    rows, channels = decay.shape
    tiles = channels // LANES
    steps = rows // SUB
    length = rows * nsp
    pitch = spaced(steps)
    me, mine = lax.axis_index("sp"), lax.axis_index("tp")

    copies = []
    for kind, (source, held) in enumerate(((decay, decay_v), (drive, drive_v), (gate, gate_v))):
        copies.append([
            pltpu.make_async_copy(
                source.at[:, pl.ds(j * LANES, LANES)], held.at[j], in_sem.at[kind, j]
            )
            for j in range(tiles)
        ])
    for j in range(tiles):
        copies[0][j].start()
        copies[1][j].start()
    for j in range(tiles):
        copies[2][j].start()
    gain_copy = pltpu.make_async_copy(gain, gain_v, gain_sem)
    gain_copy.start()

    barrier = pltpu.get_barrier_semaphore()
    for d in range(1, nsp):
        pl.semaphore_signal(barrier, inc=1, device_id={"sp": lax.rem(me + d, nsp)}, device_id_type=MESH)
    for d in range(1, ntp):
        pl.semaphore_signal(barrier, inc=1, device_id={"tp": lax.rem(mine + d, ntp)}, device_id_type=MESH)

    row = lax.broadcasted_iota(jnp.int32, (SUB, LANES), 0)
    zero = jnp.zeros((SUB, LANES), jnp.float32)
    one = jnp.ones((SUB, LANES), jnp.float32)

    def at(k):
        return pl.ds(k, SUB, stride=pitch)

    chunks = [
        (pl.ds(i * steps, steps), pl.ds(i * pitch, steps)) for i in range(SUB)
    ]

    def packed(k):
        return pl.ds(pl.multiple_of(k * SUB, SUB), SUB)

    group = min(4, tiles)
    for first in range(0, tiles, group):
        members = range(first, min(first + group, tiles))
        for j in members:
            copies[0][j].wait()
            copies[1][j].wait()
            for dense, apart in chunks:
                decay_s[j, apart, :] = jnp.exp2(decay_v[j, dense, :] * (-LOG2E / length))
                push_s[j, apart, :] = drive_v[j, dense, :].astype(jnp.float32)

        def ahead(k, carry):
            after = []
            for j, (prod, fwd, bwd) in zip(members, carry):
                keep = decay_s[j, at(k), :]
                push = push_s[j, at(k), :]
                bwd = bwd + prod * push
                prod = prod * keep
                fwd = keep * fwd + push
                fwd_s[j, packed(k), :] = fwd
                pre_s[j, packed(k), :] = prod
                after.append((prod, fwd, bwd))
            return tuple(after)

        ends = unrolled(steps, 8, ahead, tuple((one, zero, zero) for _ in members))
        for j, (prod, fwd, bwd) in zip(members, ends):
            whole, span = prod, prod
            for s in (1, 2, 4):
                keeps = row >= s
                fwd = fwd + whole * jnp.where(keeps, pltpu.roll(fwd, s, 0), 0.0)
                whole = whole * jnp.where(keeps, pltpu.roll(whole, s, 0), 1.0)
                keeps = row < SUB - s
                bwd = bwd + span * jnp.where(keeps, pltpu.roll(bwd, SUB - s, 0), 0.0)
                span = span * jnp.where(keeps, pltpu.roll(span, SUB - s, 0), 1.0)
            totals[me, 0, pl.ds(j, 1), :] = bwd[:1]
            totals[me, 1, pl.ds(j, 1), :] = whole[SUB - 1 :]
            totals[me, 2, pl.ds(j, 1), :] = fwd[SUB - 1 :]
            edge_s[0, j] = jnp.where(row >= 1, pltpu.roll(whole, 1, 0), 1.0)
            edge_s[1, j] = jnp.where(row >= 1, pltpu.roll(fwd, 1, 0), 0.0)
            edge_s[2, j] = jnp.where(row < SUB - 1, pltpu.roll(span, SUB - 1, 0), 1.0)
            edge_s[3, j] = jnp.where(row < SUB - 1, pltpu.roll(bwd, SUB - 1, 0), 0.0)

    pl.semaphore_wait(barrier, nsp + ntp - 2)

    sends = []
    for d in range(1, nsp):
        part = pl.ds(1 - (me + d) // nsp, 2)
        sends.append(pltpu.make_async_remote_copy(
            src_ref=totals.at[me, part],
            dst_ref=totals.at[me, part],
            send_sem=tsend.at[d],
            recv_sem=trecv.at[d],
            device_id={"sp": lax.rem(me + d, nsp)},
            device_id_type=MESH,
        ))
    for copy in sends:
        copy.start()

    for j in range(tiles):
        copies[2][j].wait()

        for dense, apart in chunks:
            value = gate_v[j, dense, :].astype(jnp.float32)
            sig_s[j, apart, :] = 1.0 / (1.0 + jnp.exp2(value * -LOG2E))

    for first in range(0, tiles, group):
        members = range(first, min(first + group, tiles))

        def astern(i, carry):
            k = steps - 1 - i
            after = []
            for j, (prod, bwd) in zip(members, carry):
                keep = decay_s[j, at(k), :]
                bwd = keep * bwd + push_s[j, at(k), :]
                prod = keep * prod
                sig = sig_s[j, at(k), :]
                fwd_s[j, packed(k), :] = (fwd_s[j, packed(k), :] + bwd) * sig
                pre_s[j, packed(k), :] = pre_s[j, packed(k), :] * sig
                suf_s[j, packed(k), :] = prod * sig
                after.append((prod, bwd))
            return tuple(after)

        unrolled(steps, 8, astern, tuple((one, zero) for _ in members))

    for copy in sends:
        copy.wait()

    enter_f = jnp.zeros((tiles, LANES), jnp.float32)
    enter_b = jnp.zeros((tiles, LANES), jnp.float32)
    for s in range(nsp - 1):
        enter_f = jnp.where(s < me, totals[s, 1] * enter_f + totals[s, 2], enter_f)
        e = nsp - 1 - s
        enter_b = jnp.where(e > me, totals[e, 1] * enter_b + totals[e, 0], enter_b)
    start_f = [edge_s[0, j] * enter_f[j : j + 1] + edge_s[1, j] for j in range(tiles)]
    start_b = [edge_s[2, j] * enter_b[j : j + 1] + edge_s[3, j] for j in range(tiles)]

    width = powers.shape[-1]
    lane = lax.broadcasted_iota(jnp.int32, (SUB, width), 1)

    def finish(k, sums):
        squares = zero
        for j in range(tiles):
            gated = (
                fwd_s[j, packed(k), :]
                + pre_s[j, packed(k), :] * start_f[j]
                + suf_s[j, packed(k), :] * start_b[j]
            )
            gated_s[j, at(k), :] = gated
            squares = squares + gated * gated
        return jnp.where(lane == k, jnp.sum(squares, axis=1, keepdims=True), sums)

    powers[mine] = unrolled(steps, 8, finish, jnp.zeros((SUB, width), jnp.float32))

    sends = []
    for d in range(1, ntp):
        sends.append(pltpu.make_async_remote_copy(
            src_ref=powers.at[mine],
            dst_ref=powers.at[mine],
            send_sem=psend.at[d],
            recv_sem=precv.at[d],
            device_id={"tp": lax.rem(mine + d, ntp)},
            device_id_type=MESH,
        ))
    for copy in sends:
        copy.start()
    for copy in sends:
        copy.wait()

    power = powers[0]
    for s in range(1, ntp):
        power = power + powers[s]
    power = power * (1.0 / (length * channels * ntp))
    inverse = lax.rsqrt(power + 1e-06) * length ** (-0.5)
    for k in range(steps):
        inv_s[at(k), :] = jnp.broadcast_to(inverse[:, k : k + 1], (SUB, LANES))

    gain_copy.wait()

    def emit(j, carry):
        columns = pl.ds(pl.multiple_of(j * LANES, LANES), LANES)
        own = gain_v[pl.ds(j, 1), :]
        for dense, apart in chunks:
            out[dense, columns] = (gated_s[j, apart, :] * inv_s[apart, :] * own).astype(jnp.bfloat16)
        return carry

    lax.fori_loop(0, tiles, emit, 0)


def body(nsp, ntp, decay_rate, drive_in, gate_in, norm_gain):
    batch, rows, channels = decay_rate.shape
    tiles = channels // LANES
    steps = rows // SUB
    width = -(-steps // LANES) * LANES
    plane = pltpu.VMEM((tiles, rows, LANES), jnp.float32)
    wide = pltpu.VMEM((tiles, SUB * spaced(steps), LANES), jnp.float32)
    half = pltpu.VMEM((tiles, rows, LANES), jnp.bfloat16)
    outside = pl.BlockSpec(memory_space=pltpu.HBM)
    vmem = pl.BlockSpec(memory_space=pltpu.VMEM)
    result = pl.pallas_call(
        functools.partial(kernel, nsp, ntp),
        out_shape=jax.ShapeDtypeStruct((rows, channels), jnp.bfloat16),
        in_specs=[outside] * 4,
        out_specs=vmem,
        scratch_shapes=[
            plane, half, half, wide, wide, wide, plane, plane, plane, wide,
            pltpu.VMEM((SUB * spaced(steps), LANES), jnp.float32),
            pltpu.VMEM((4, tiles, SUB, LANES), jnp.float32),
            pltpu.VMEM((nsp, 3, tiles, LANES), jnp.float32),
            pltpu.VMEM((ntp, SUB, width), jnp.float32),
            pltpu.VMEM((tiles, LANES), jnp.float32),
            pltpu.SemaphoreType.DMA,
            pltpu.SemaphoreType.DMA((3, tiles)),
            pltpu.SemaphoreType.DMA((nsp,)),
            pltpu.SemaphoreType.DMA((nsp,)),
            pltpu.SemaphoreType.DMA((ntp,)),
            pltpu.SemaphoreType.DMA((ntp,)),
        ],
        compiler_params=pltpu.CompilerParams(
            collective_id=0, has_side_effects=True, vmem_limit_bytes=52 * 1024 * 1024
        ),
    )(
        decay_rate.reshape(rows, channels),
        drive_in.reshape(rows, channels),
        gate_in.reshape(rows, channels),
        norm_gain.reshape(tiles, LANES),
    )
    return result.reshape(batch, rows, channels)


def solution(mesh):
    in_specs = (P(None, "sp", "tp"), P(None, "sp", "tp"), P(None, "sp", "tp"), P("tp"))
    out_specs = P(None, "sp", "tp")
    local = functools.partial(body, mesh.shape["sp"], mesh.shape["tp"])
    return jax.shard_map(local, mesh=mesh, in_specs=in_specs, out_specs=out_specs, check_vma=False)
```

```python
import functools

import jax
import jax.numpy as jnp
from jax import lax
from jax.experimental import pallas as pl
from jax.experimental.pallas import tpu as pltpu
from jax.sharding import PartitionSpec as P

LANES = 128
SUB = 8
LOG2E = 1.4426950408889634
MESH = pl.DeviceIdType.MESH


def unrolled(count, by, step, carry):
    by = next(size for size in range(min(by, count), 0, -1) if count % size == 0)

    def block(outer, carry):
        for inner in range(by):
            carry = step(outer * by + inner, carry)
        return carry

    return lax.fori_loop(0, count // by, block, carry)


def spaced(steps):
    return steps + next(more for more in range(4, 40, 4) if (steps + more) % 8 == 4)


def kernel(
    nsp, ntp, decay, drive, gate, gain, out,
    decay_v, drive_v, gate_v, decay_s, push_s, sig_s, fwd_s, pre_s, suf_s, gated_s,
    inv_s, edge_s, totals, powers, gain_v, gain_sem, in_sem, tsend, trecv, psend, precv,
):
    rows, channels = decay.shape
    tiles = channels // LANES
    steps = rows // SUB
    length = rows * nsp
    pitch = spaced(steps)
    me, mine = lax.axis_index("sp"), lax.axis_index("tp")

    copies = []
    for kind, (source, held) in enumerate(((decay, decay_v), (drive, drive_v), (gate, gate_v))):
        copies.append([
            pltpu.make_async_copy(
                source.at[:, pl.ds(j * LANES, LANES)], held.at[j], in_sem.at[kind, j]
            )
            for j in range(tiles)
        ])
    for j in range(tiles):
        copies[0][j].start()
        copies[1][j].start()
    for j in range(tiles):
        copies[2][j].start()
    gain_copy = pltpu.make_async_copy(gain, gain_v, gain_sem)
    gain_copy.start()

    barrier = pltpu.get_barrier_semaphore()
    for d in range(1, nsp):
        pl.semaphore_signal(barrier, inc=1, device_id={"sp": lax.rem(me + d, nsp)}, device_id_type=MESH)
    for d in range(1, ntp):
        pl.semaphore_signal(barrier, inc=1, device_id={"tp": lax.rem(mine + d, ntp)}, device_id_type=MESH)

    row = lax.broadcasted_iota(jnp.int32, (SUB, LANES), 0)
    zero = jnp.zeros((SUB, LANES), jnp.float32)
    one = jnp.ones((SUB, LANES), jnp.float32)

    def at(k):
        return pl.ds(k, SUB, stride=pitch)

    chunks = [
        (pl.ds(i * steps, steps), pl.ds(i * pitch, steps)) for i in range(SUB)
    ]

    def packed(k):
        return pl.ds(pl.multiple_of(k * SUB, SUB), SUB)

    group = min(4, tiles)
    for first in range(0, tiles, group):
        members = range(first, min(first + group, tiles))
        for j in members:
            copies[0][j].wait()
            copies[1][j].wait()
            for dense, apart in chunks:
                decay_s[j, apart, :] = jnp.exp2(decay_v[j, dense, :] * (-LOG2E / length))
                push_s[j, apart, :] = drive_v[j, dense, :].astype(jnp.float32)

        def ahead(k, carry):
            after = []
            for j, (prod, fwd, bwd) in zip(members, carry):
                keep = decay_s[j, at(k), :]
                push = push_s[j, at(k), :]
                bwd = bwd + prod * push
                prod = prod * keep
                fwd = keep * fwd + push
                fwd_s[j, packed(k), :] = fwd
                pre_s[j, packed(k), :] = prod
                after.append((prod, fwd, bwd))
            return tuple(after)

        ends = unrolled(steps, 8, ahead, tuple((one, zero, zero) for _ in members))
        for j, (prod, fwd, bwd) in zip(members, ends):
            whole, span = prod, prod
            for s in (1, 2, 4):
                keeps = row >= s
                fwd = fwd + whole * jnp.where(keeps, pltpu.roll(fwd, s, 0), 0.0)
                whole = whole * jnp.where(keeps, pltpu.roll(whole, s, 0), 1.0)
                keeps = row < SUB - s
                bwd = bwd + span * jnp.where(keeps, pltpu.roll(bwd, SUB - s, 0), 0.0)
                span = span * jnp.where(keeps, pltpu.roll(span, SUB - s, 0), 1.0)
            totals[me, 0, pl.ds(j, 1), :] = bwd[:1]
            totals[me, 1, pl.ds(j, 1), :] = whole[SUB - 1 :]
            totals[me, 2, pl.ds(j, 1), :] = fwd[SUB - 1 :]
            edge_s[0, j] = jnp.where(row >= 1, pltpu.roll(whole, 1, 0), 1.0)
            edge_s[1, j] = jnp.where(row >= 1, pltpu.roll(fwd, 1, 0), 0.0)
            edge_s[2, j] = jnp.where(row < SUB - 1, pltpu.roll(span, SUB - 1, 0), 1.0)
            edge_s[3, j] = jnp.where(row < SUB - 1, pltpu.roll(bwd, SUB - 1, 0), 0.0)

    pl.semaphore_wait(barrier, nsp + ntp - 2)

    sends = []
    ahead_first = (2 * me + 1) // nsp
    for i in range(nsp - 1):
        high = nsp - 1 - i - (i + me + 1) // nsp
        low = i + (nsp - 1 - me + i + 1) // nsp
        peer = high * (1 - ahead_first) + low * ahead_first
        d = lax.rem(peer - me + nsp, nsp)
        part = pl.ds(1 - (me + d) // nsp, 2)
        sends.append(pltpu.make_async_remote_copy(
            src_ref=totals.at[me, part],
            dst_ref=totals.at[me, part],
            send_sem=tsend.at[d],
            recv_sem=trecv.at[d],
            device_id={"sp": peer},
            device_id_type=MESH,
        ))
    for copy in sends:
        copy.start()

    for j in range(tiles):
        copies[2][j].wait()

        for dense, apart in chunks:
            value = gate_v[j, dense, :].astype(jnp.float32)
            sig_s[j, apart, :] = 1.0 / (1.0 + jnp.exp2(value * -LOG2E))

    for first in range(0, tiles, group):
        members = range(first, min(first + group, tiles))

        def astern(i, carry):
            k = steps - 1 - i
            after = []
            for j, (prod, bwd) in zip(members, carry):
                keep = decay_s[j, at(k), :]
                bwd = keep * bwd + push_s[j, at(k), :]
                prod = keep * prod
                sig = sig_s[j, at(k), :]
                fwd_s[j, packed(k), :] = (fwd_s[j, packed(k), :] + bwd) * sig
                pre_s[j, packed(k), :] = pre_s[j, packed(k), :] * sig
                suf_s[j, packed(k), :] = prod * sig
                after.append((prod, bwd))
            return tuple(after)

        unrolled(steps, 8, astern, tuple((one, zero) for _ in members))

    for copy in sends:
        copy.wait()

    enter_f = jnp.zeros((tiles, LANES), jnp.float32)
    enter_b = jnp.zeros((tiles, LANES), jnp.float32)
    for s in range(nsp - 1):
        enter_f = jnp.where(s < me, totals[s, 1] * enter_f + totals[s, 2], enter_f)
        e = nsp - 1 - s
        enter_b = jnp.where(e > me, totals[e, 1] * enter_b + totals[e, 0], enter_b)
    start_f = [edge_s[0, j] * enter_f[j : j + 1] + edge_s[1, j] for j in range(tiles)]
    start_b = [edge_s[2, j] * enter_b[j : j + 1] + edge_s[3, j] for j in range(tiles)]

    width = powers.shape[-1]
    lane = lax.broadcasted_iota(jnp.int32, (SUB, width), 1)

    def finish(k, sums):
        squares = zero
        for j in range(tiles):
            gated = (
                fwd_s[j, packed(k), :]
                + pre_s[j, packed(k), :] * start_f[j]
                + suf_s[j, packed(k), :] * start_b[j]
            )
            gated_s[j, at(k), :] = gated
            squares = squares + gated * gated
        return jnp.where(lane == k, jnp.sum(squares, axis=1, keepdims=True), sums)

    powers[mine] = unrolled(steps, 8, finish, jnp.zeros((SUB, width), jnp.float32))

    sends = []
    for d in range(1, ntp):
        sends.append(pltpu.make_async_remote_copy(
            src_ref=powers.at[mine],
            dst_ref=powers.at[mine],
            send_sem=psend.at[d],
            recv_sem=precv.at[d],
            device_id={"tp": lax.rem(mine + d, ntp)},
            device_id_type=MESH,
        ))
    for copy in sends:
        copy.start()
    for copy in sends:
        copy.wait()

    power = powers[0]
    for s in range(1, ntp):
        power = power + powers[s]
    power = power * (1.0 / (length * channels * ntp))
    inverse = lax.rsqrt(power + 1e-06) * length ** (-0.5)
    for k in range(steps):
        inv_s[at(k), :] = jnp.broadcast_to(inverse[:, k : k + 1], (SUB, LANES))

    gain_copy.wait()

    def emit(j, carry):
        columns = pl.ds(pl.multiple_of(j * LANES, LANES), LANES)
        own = gain_v[pl.ds(j, 1), :]
        for dense, apart in chunks:
            out[dense, columns] = (gated_s[j, apart, :] * inv_s[apart, :] * own).astype(jnp.bfloat16)
        return carry

    lax.fori_loop(0, tiles, emit, 0)


def body(nsp, ntp, decay_rate, drive_in, gate_in, norm_gain):
    batch, rows, channels = decay_rate.shape
    tiles = channels // LANES
    steps = rows // SUB
    width = -(-steps // LANES) * LANES
    plane = pltpu.VMEM((tiles, rows, LANES), jnp.float32)
    wide = pltpu.VMEM((tiles, SUB * spaced(steps), LANES), jnp.float32)
    half = pltpu.VMEM((tiles, rows, LANES), jnp.bfloat16)
    outside = pl.BlockSpec(memory_space=pltpu.HBM)
    vmem = pl.BlockSpec(memory_space=pltpu.VMEM)
    result = pl.pallas_call(
        functools.partial(kernel, nsp, ntp),
        out_shape=jax.ShapeDtypeStruct((rows, channels), jnp.bfloat16),
        in_specs=[outside] * 4,
        out_specs=vmem,
        scratch_shapes=[
            plane, half, half, wide, wide, wide, plane, plane, plane, wide,
            pltpu.VMEM((SUB * spaced(steps), LANES), jnp.float32),
            pltpu.VMEM((4, tiles, SUB, LANES), jnp.float32),
            pltpu.VMEM((nsp, 3, tiles, LANES), jnp.float32),
            pltpu.VMEM((ntp, SUB, width), jnp.float32),
            pltpu.VMEM((tiles, LANES), jnp.float32),
            pltpu.SemaphoreType.DMA,
            pltpu.SemaphoreType.DMA((3, tiles)),
            pltpu.SemaphoreType.DMA((nsp,)),
            pltpu.SemaphoreType.DMA((nsp,)),
            pltpu.SemaphoreType.DMA((ntp,)),
            pltpu.SemaphoreType.DMA((ntp,)),
        ],
        compiler_params=pltpu.CompilerParams(
            collective_id=0, has_side_effects=True, vmem_limit_bytes=52 * 1024 * 1024
        ),
    )(*(
        pltpu.with_memory_space_constraint(value, pltpu.HBM)
        for value in (
            decay_rate.reshape(rows, channels),
            drive_in.reshape(rows, channels),
            gate_in.reshape(rows, channels),
            norm_gain.reshape(tiles, LANES),
        )
    ))
    return result.reshape(batch, rows, channels)


def solution(mesh):
    in_specs = (P(None, "sp", "tp"), P(None, "sp", "tp"), P(None, "sp", "tp"), P("tp"))
    out_specs = P(None, "sp", "tp")
    local = functools.partial(body, mesh.shape["sp"], mesh.shape["tp"])
    return jax.shard_map(local, mesh=mesh, in_specs=in_specs, out_specs=out_specs, check_vma=False)
```

```python
import functools

import jax
import jax.numpy as jnp
from jax import lax
from jax.experimental import pallas as pl
from jax.experimental.pallas import tpu as pltpu
from jax.sharding import PartitionSpec as P

LANES = 128
SUB = 8
LOG2E = 1.4426950408889634
MESH = pl.DeviceIdType.MESH


def unrolled(count, by, step, carry):
    by = next(size for size in range(min(by, count), 0, -1) if count % size == 0)

    def block(outer, carry):
        for inner in range(by):
            carry = step(outer * by + inner, carry)
        return carry

    return lax.fori_loop(0, count // by, block, carry)


def spaced(steps):
    return steps + next(more for more in range(4, 40, 4) if (steps + more) % 8 == 4)


def kernel(
    nsp, ntp, decay, drive, gate, gain, gated_s, inverse,
    decay_v, drive_v, gate_v, decay_s, push_s, sig_s, fwd_s, pre_s, suf_s,
    edge_s, totals, powers, gain_v, gain_sem, in_sem, tsend, trecv, psend, precv,
):
    rows, channels = decay.shape
    tiles = channels // LANES
    steps = rows // SUB
    length = rows * nsp
    pitch = spaced(steps)
    me, mine = lax.axis_index("sp"), lax.axis_index("tp")

    barrier = pltpu.get_barrier_semaphore()
    for d in range(1, nsp):
        pl.semaphore_signal(barrier, inc=1, device_id={"sp": lax.rem(me + d, nsp)}, device_id_type=MESH)
    for d in range(1, ntp):
        pl.semaphore_signal(barrier, inc=1, device_id={"tp": lax.rem(mine + d, ntp)}, device_id_type=MESH)

    copies = []
    for kind, (source, held) in enumerate(((decay, decay_v), (drive, drive_v), (gate, gate_v))):
        copies.append([
            pltpu.make_async_copy(
                source.at[:, pl.ds(j * LANES, LANES)], held.at[j], in_sem.at[kind, j]
            )
            for j in range(tiles)
        ])
    for j in range(tiles):
        copies[0][j].start()
        copies[1][j].start()
    for j in range(tiles):
        copies[2][j].start()
    gain_copy = pltpu.make_async_copy(gain, gain_v, gain_sem)
    gain_copy.start()

    row = lax.broadcasted_iota(jnp.int32, (SUB, LANES), 0)
    zero = jnp.zeros((SUB, LANES), jnp.float32)
    one = jnp.ones((SUB, LANES), jnp.float32)

    def at(k):
        return pl.ds(k, SUB, stride=pitch)

    chunks = [
        (pl.ds(i * steps, steps), pl.ds(i * pitch, steps)) for i in range(SUB)
    ]

    def packed(k):
        return pl.ds(pl.multiple_of(k * SUB, SUB), SUB)

    group = min(4, tiles)
    for first in range(0, tiles, group):
        members = range(first, min(first + group, tiles))
        for j in members:
            copies[0][j].wait()
            copies[1][j].wait()
            for dense, apart in chunks:
                decay_s[j, apart, :] = jnp.exp2(decay_v[j, dense, :] * (-LOG2E / length))
                push_s[j, apart, :] = drive_v[j, dense, :].astype(jnp.float32)

        def ahead(k, carry):
            after = []
            for j, (prod, fwd, bwd) in zip(members, carry):
                keep = decay_s[j, at(k), :]
                push = push_s[j, at(k), :]
                bwd = bwd + prod * push
                prod = prod * keep
                fwd = keep * fwd + push
                fwd_s[j, packed(k), :] = fwd
                pre_s[j, packed(k), :] = prod
                after.append((prod, fwd, bwd))
            return tuple(after)

        ends = unrolled(steps, 8, ahead, tuple((one, zero, zero) for _ in members))
        for j, (prod, fwd, bwd) in zip(members, ends):
            whole, span = prod, prod
            for s in (1, 2, 4):
                keeps = row >= s
                fwd = fwd + whole * jnp.where(keeps, pltpu.roll(fwd, s, 0), 0.0)
                whole = whole * jnp.where(keeps, pltpu.roll(whole, s, 0), 1.0)
                keeps = row < SUB - s
                bwd = bwd + span * jnp.where(keeps, pltpu.roll(bwd, SUB - s, 0), 0.0)
                span = span * jnp.where(keeps, pltpu.roll(span, SUB - s, 0), 1.0)
            totals[me, 0, pl.ds(j, 1), :] = bwd[:1]
            totals[me, 1, pl.ds(j, 1), :] = whole[SUB - 1 :]
            totals[me, 2, pl.ds(j, 1), :] = fwd[SUB - 1 :]
            edge_s[0, j] = jnp.where(row >= 1, pltpu.roll(whole, 1, 0), 1.0)
            edge_s[1, j] = jnp.where(row >= 1, pltpu.roll(fwd, 1, 0), 0.0)
            edge_s[2, j] = jnp.where(row < SUB - 1, pltpu.roll(span, SUB - 1, 0), 1.0)
            edge_s[3, j] = jnp.where(row < SUB - 1, pltpu.roll(bwd, SUB - 1, 0), 0.0)

    pl.semaphore_wait(barrier, nsp + ntp - 2)

    sends = []
    ahead_first = (2 * me + 1) // nsp
    for i in range(nsp - 1):
        high = nsp - 1 - i - (i + me + 1) // nsp
        low = i + (nsp - 1 - me + i + 1) // nsp
        peer = high * (1 - ahead_first) + low * ahead_first
        d = lax.rem(peer - me + nsp, nsp)
        part = pl.ds(1 - (me + d) // nsp, 2)
        sends.append(pltpu.make_async_remote_copy(
            src_ref=totals.at[me, part],
            dst_ref=totals.at[me, part],
            send_sem=tsend.at[d],
            recv_sem=trecv.at[d],
            device_id={"sp": peer},
            device_id_type=MESH,
        ))
    for copy in sends:
        copy.start()

    for j in range(tiles):
        copies[2][j].wait()

        for dense, apart in chunks:
            value = gate_v[j, dense, :].astype(jnp.float32)
            sig_s[j, apart, :] = 1.0 / (1.0 + jnp.exp2(value * -LOG2E))

    for first in range(0, tiles, group):
        members = range(first, min(first + group, tiles))

        def astern(i, carry):
            k = steps - 1 - i
            after = []
            for j, (prod, bwd) in zip(members, carry):
                keep = decay_s[j, at(k), :]
                bwd = keep * bwd + push_s[j, at(k), :]
                prod = keep * prod
                sig = sig_s[j, at(k), :]
                fwd_s[j, packed(k), :] = (fwd_s[j, packed(k), :] + bwd) * sig
                pre_s[j, packed(k), :] = pre_s[j, packed(k), :] * sig
                suf_s[j, packed(k), :] = prod * sig
                after.append((prod, bwd))
            return tuple(after)

        unrolled(steps, 8, astern, tuple((one, zero) for _ in members))

    for copy in sends:
        copy.wait()

    enter_f = jnp.zeros((tiles, LANES), jnp.float32)
    enter_b = jnp.zeros((tiles, LANES), jnp.float32)
    for s in range(nsp - 1):
        enter_f = jnp.where(s < me, totals[s, 1] * enter_f + totals[s, 2], enter_f)
        e = nsp - 1 - s
        enter_b = jnp.where(e > me, totals[e, 1] * enter_b + totals[e, 0], enter_b)
    start_f = [edge_s[0, j] * enter_f[j : j + 1] + edge_s[1, j] for j in range(tiles)]
    start_b = [edge_s[2, j] * enter_b[j : j + 1] + edge_s[3, j] for j in range(tiles)]

    width = powers.shape[-1]
    lane = lax.broadcasted_iota(jnp.int32, (SUB, width), 1)

    def finish(k, sums):
        squares = zero
        for j in range(tiles):
            gated = (
                fwd_s[j, packed(k), :]
                + pre_s[j, packed(k), :] * start_f[j]
                + suf_s[j, packed(k), :] * start_b[j]
            )
            gated_s[j, at(k), :] = gated
            squares = squares + gated * gated
        return jnp.where(lane == k, jnp.sum(squares, axis=1, keepdims=True), sums)

    powers[mine] = unrolled(steps, 8, finish, jnp.zeros((SUB, width), jnp.float32))

    sends = []
    for d in range(1, ntp):
        sends.append(pltpu.make_async_remote_copy(
            src_ref=powers.at[mine],
            dst_ref=powers.at[mine],
            send_sem=psend.at[d],
            recv_sem=precv.at[d],
            device_id={"tp": lax.rem(mine + d, ntp)},
            device_id_type=MESH,
        ))
    for copy in sends:
        copy.start()
    gain_copy.wait()

    def weigh(j, carry):
        own = gain_v[pl.ds(j, 1), :]
        for _, apart in chunks:
            gated_s[j, apart, :] = gated_s[j, apart, :] * own
        return carry

    lax.fori_loop(0, tiles, weigh, 0)

    for copy in sends:
        copy.wait()

    power = powers[0]
    for s in range(1, ntp):
        power = power + powers[s]
    power = power * (1.0 / (length * channels * ntp))
    inverse[...] = lax.rsqrt(power + 1e-06) * length ** (-0.5)


def emit(gated, inverse, out, inv_s, staged, sems):
    rows, channels = out.shape
    tiles = channels // LANES
    steps = rows // SUB
    pitch = spaced(steps)
    scale = inverse[...]
    for k in range(steps):
        inv_s[pl.ds(k, SUB, stride=pitch), :] = jnp.broadcast_to(scale[:, k : k + 1], (SUB, LANES))
    copies = []
    for i in range(SUB):
        dense, apart = pl.ds(i * steps, steps), pl.ds(i * pitch, steps)
        for j in range(tiles):
            staged[dense, pl.ds(j * LANES, LANES)] = (
                gated[j, apart, :] * inv_s[apart, :]
            ).astype(jnp.bfloat16)
        copies.append(pltpu.make_async_copy(staged.at[dense], out.at[dense], sems.at[i]))
        copies[-1].start()
    for copy in copies:
        copy.wait()


def body(nsp, ntp, decay_rate, drive_in, gate_in, norm_gain):
    batch, rows, channels = decay_rate.shape
    tiles = channels // LANES
    steps = rows // SUB
    width = -(-steps // LANES) * LANES
    plane = pltpu.VMEM((tiles, rows, LANES), jnp.float32)
    wide = pltpu.VMEM((tiles, SUB * spaced(steps), LANES), jnp.float32)
    half = pltpu.VMEM((tiles, rows, LANES), jnp.bfloat16)
    outside = pl.BlockSpec(memory_space=pltpu.HBM)
    vmem = pl.BlockSpec(memory_space=pltpu.VMEM)
    gated, inverse = pl.pallas_call(
        functools.partial(kernel, nsp, ntp),
        out_shape=(
            pltpu.VMEM((tiles, SUB * spaced(steps), LANES), jnp.float32),
            pltpu.VMEM((SUB, width), jnp.float32),
        ),
        in_specs=[outside] * 4,
        out_specs=(vmem, vmem),
        scratch_shapes=[
            plane, half, half, wide, wide, wide, plane, plane, plane,
            pltpu.VMEM((4, tiles, SUB, LANES), jnp.float32),
            pltpu.VMEM((nsp, 3, tiles, LANES), jnp.float32),
            pltpu.VMEM((ntp, SUB, width), jnp.float32),
            pltpu.VMEM((tiles, LANES), jnp.float32),
            pltpu.SemaphoreType.DMA,
            pltpu.SemaphoreType.DMA((3, tiles)),
            pltpu.SemaphoreType.DMA((nsp,)),
            pltpu.SemaphoreType.DMA((nsp,)),
            pltpu.SemaphoreType.DMA((ntp,)),
            pltpu.SemaphoreType.DMA((ntp,)),
        ],
        compiler_params=pltpu.CompilerParams(
            collective_id=0, has_side_effects=True, vmem_limit_bytes=52 * 1024 * 1024
        ),
    )(*(
        pltpu.with_memory_space_constraint(value, pltpu.HBM)
        for value in (
            decay_rate.reshape(rows, channels),
            drive_in.reshape(rows, channels),
            gate_in.reshape(rows, channels),
            norm_gain.reshape(tiles, LANES),
        )
    ))
    result = pl.pallas_call(
        emit,
        out_shape=jax.ShapeDtypeStruct((rows, channels), jnp.bfloat16),
        in_specs=[vmem, vmem],
        out_specs=outside,
        scratch_shapes=[
            pltpu.VMEM((SUB * spaced(steps), LANES), jnp.float32),
            pltpu.VMEM((rows, channels), jnp.bfloat16),
            pltpu.SemaphoreType.DMA((SUB,)),
        ],
        compiler_params=pltpu.CompilerParams(vmem_limit_bytes=32 * 1024 * 1024),
    )(
        pltpu.with_memory_space_constraint(gated, pltpu.VMEM),
        pltpu.with_memory_space_constraint(inverse, pltpu.VMEM),
    )
    return result.reshape(batch, rows, channels)


def solution(mesh):
    in_specs = (P(None, "sp", "tp"), P(None, "sp", "tp"), P(None, "sp", "tp"), P("tp"))
    out_specs = P(None, "sp", "tp")
    local = functools.partial(body, mesh.shape["sp"], mesh.shape["tp"])
    return jax.shard_map(local, mesh=mesh, in_specs=in_specs, out_specs=out_specs, check_vma=False)
```

```python
import functools

import jax
import jax.numpy as jnp
from jax import lax
from jax.experimental import pallas as pl
from jax.experimental.pallas import tpu as pltpu
from jax.sharding import PartitionSpec as P

LANES = 128
SUB = 8
LOG2E = 1.4426950408889634
MESH = pl.DeviceIdType.MESH


def unrolled(count, by, step, carry):
    by = next(size for size in range(min(by, count), 0, -1) if count % size == 0)

    def block(outer, carry):
        for inner in range(by):
            carry = step(outer * by + inner, carry)
        return carry

    return lax.fori_loop(0, count // by, block, carry)


def spaced(steps):
    return steps + next(more for more in range(4, 40, 4) if (steps + more) % 8 == 4)


def kernel(
    nsp, ntp, decay, drive, gate, gain, gated_s, inverse,
    decay_v, drive_v, gate_v, decay_s, push_s, sig_s, fwd_s, pre_s, suf_s,
    edge_s, totals, powers, gain_v, gain_sem, in_sem, tsend, trecv, psend, precv,
):
    rows, channels = decay.shape
    tiles = channels // LANES
    steps = rows // SUB
    length = rows * nsp
    pitch = spaced(steps)
    me, mine = lax.axis_index("sp"), lax.axis_index("tp")

    barrier = pltpu.get_barrier_semaphore()
    ahead_first = (2 * me + 1) // nsp
    for i in range(nsp - 1):
        high = nsp - 1 - i - (i + me + 1) // nsp
        low = i + (nsp - 1 - me + i + 1) // nsp
        peer = high * (1 - ahead_first) + low * ahead_first
        pl.semaphore_signal(barrier, inc=1, device_id={"sp": peer}, device_id_type=MESH)
    for d in range(1, ntp):
        pl.semaphore_signal(barrier, inc=1, device_id={"tp": lax.rem(mine + d, ntp)}, device_id_type=MESH)

    copies = []
    for kind, (source, held) in enumerate(((decay, decay_v), (drive, drive_v), (gate, gate_v))):
        copies.append([
            pltpu.make_async_copy(
                source.at[:, pl.ds(j * LANES, LANES)], held.at[j], in_sem.at[kind, j]
            )
            for j in range(tiles)
        ])
    for j in range(tiles):
        copies[0][j].start()
        copies[1][j].start()
    for j in range(tiles):
        copies[2][j].start()
    gain_copy = pltpu.make_async_copy(gain, gain_v, gain_sem)
    gain_copy.start()

    row = lax.broadcasted_iota(jnp.int32, (SUB, LANES), 0)
    zero = jnp.zeros((SUB, LANES), jnp.float32)
    one = jnp.ones((SUB, LANES), jnp.float32)

    def at(k):
        return pl.ds(k, SUB, stride=pitch)

    chunks = [
        (pl.ds(i * steps, steps), pl.ds(i * pitch, steps)) for i in range(SUB)
    ]

    def packed(k):
        return pl.ds(pl.multiple_of(k * SUB, SUB), SUB)

    group = min(4, tiles)
    for first in range(0, tiles, group):
        members = range(first, min(first + group, tiles))
        for j in members:
            copies[0][j].wait()
            copies[1][j].wait()
            for dense, apart in chunks:
                decay_s[j, apart, :] = jnp.exp2(decay_v[j, dense, :] * (-LOG2E / length))
                push_s[j, apart, :] = drive_v[j, dense, :].astype(jnp.float32)

        def ahead(k, carry):
            after = []
            for j, (prod, fwd, bwd) in zip(members, carry):
                keep = decay_s[j, at(k), :]
                push = push_s[j, at(k), :]
                bwd = bwd + prod * push
                prod = prod * keep
                fwd = keep * fwd + push
                fwd_s[j, packed(k), :] = fwd
                pre_s[j, packed(k), :] = prod
                after.append((prod, fwd, bwd))
            return tuple(after)

        ends = unrolled(steps, 8, ahead, tuple((one, zero, zero) for _ in members))
        for j, (prod, fwd, bwd) in zip(members, ends):
            whole, span = prod, prod
            for s in (1, 2, 4):
                keeps = row >= s
                fwd = fwd + whole * jnp.where(keeps, pltpu.roll(fwd, s, 0), 0.0)
                whole = whole * jnp.where(keeps, pltpu.roll(whole, s, 0), 1.0)
                keeps = row < SUB - s
                bwd = bwd + span * jnp.where(keeps, pltpu.roll(bwd, SUB - s, 0), 0.0)
                span = span * jnp.where(keeps, pltpu.roll(span, SUB - s, 0), 1.0)
            totals[me, 0, pl.ds(j, 1), :] = bwd[:1]
            totals[me, 1, pl.ds(j, 1), :] = whole[SUB - 1 :]
            totals[me, 2, pl.ds(j, 1), :] = fwd[SUB - 1 :]
            edge_s[0, j] = jnp.where(row >= 1, pltpu.roll(whole, 1, 0), 1.0)
            edge_s[1, j] = jnp.where(row >= 1, pltpu.roll(fwd, 1, 0), 0.0)
            edge_s[2, j] = jnp.where(row < SUB - 1, pltpu.roll(span, SUB - 1, 0), 1.0)
            edge_s[3, j] = jnp.where(row < SUB - 1, pltpu.roll(bwd, SUB - 1, 0), 0.0)

    pl.semaphore_wait(barrier, nsp + ntp - 2)

    sends = []
    ahead_first = (2 * me + 1) // nsp
    for i in range(nsp - 1):
        high = nsp - 1 - i - (i + me + 1) // nsp
        low = i + (nsp - 1 - me + i + 1) // nsp
        peer = high * (1 - ahead_first) + low * ahead_first
        d = lax.rem(peer - me + nsp, nsp)
        part = pl.ds(1 - (me + d) // nsp, 2)
        sends.append(pltpu.make_async_remote_copy(
            src_ref=totals.at[me, part],
            dst_ref=totals.at[me, part],
            send_sem=tsend.at[d],
            recv_sem=trecv.at[d],
            device_id={"sp": peer},
            device_id_type=MESH,
        ))
    for copy in sends:
        copy.start()

    for j in range(tiles):
        copies[2][j].wait()

        for dense, apart in chunks:
            value = gate_v[j, dense, :].astype(jnp.float32)
            sig_s[j, apart, :] = 1.0 / (1.0 + jnp.exp2(value * -LOG2E))

    for first in range(0, tiles, group):
        members = range(first, min(first + group, tiles))

        def astern(i, carry):
            k = steps - 1 - i
            after = []
            for j, (prod, bwd) in zip(members, carry):
                keep = decay_s[j, at(k), :]
                bwd = keep * bwd + push_s[j, at(k), :]
                prod = keep * prod
                sig = sig_s[j, at(k), :]
                fwd_s[j, packed(k), :] = (fwd_s[j, packed(k), :] + bwd) * sig
                pre_s[j, packed(k), :] = pre_s[j, packed(k), :] * sig
                suf_s[j, packed(k), :] = prod * sig
                after.append((prod, bwd))
            return tuple(after)

        unrolled(steps, 8, astern, tuple((one, zero) for _ in members))

    for copy in sends:
        copy.wait()

    enter_f = jnp.zeros((tiles, LANES), jnp.float32)
    enter_b = jnp.zeros((tiles, LANES), jnp.float32)
    for s in range(nsp - 1):
        enter_f = jnp.where(s < me, totals[s, 1] * enter_f + totals[s, 2], enter_f)
        e = nsp - 1 - s
        enter_b = jnp.where(e > me, totals[e, 1] * enter_b + totals[e, 0], enter_b)
    start_f = [edge_s[0, j] * enter_f[j : j + 1] + edge_s[1, j] for j in range(tiles)]
    start_b = [edge_s[2, j] * enter_b[j : j + 1] + edge_s[3, j] for j in range(tiles)]

    width = powers.shape[-1]
    lane = lax.broadcasted_iota(jnp.int32, (SUB, width), 1)

    def finish(k, sums):
        squares = zero
        for j in range(tiles):
            gated = (
                fwd_s[j, packed(k), :]
                + pre_s[j, packed(k), :] * start_f[j]
                + suf_s[j, packed(k), :] * start_b[j]
            )
            gated_s[j, at(k), :] = gated
            squares = squares + gated * gated
        return jnp.where(lane == k, jnp.sum(squares, axis=1, keepdims=True), sums)

    powers[mine] = unrolled(steps, 64, finish, jnp.zeros((SUB, width), jnp.float32))

    sends = []
    for d in sorted(range(1, ntp), key=lambda d: abs(2 * d - ntp)):
        sends.append(pltpu.make_async_remote_copy(
            src_ref=powers.at[mine],
            dst_ref=powers.at[mine],
            send_sem=psend.at[d],
            recv_sem=precv.at[d],
            device_id={"tp": lax.rem(mine + d, ntp)},
            device_id_type=MESH,
        ))
    for copy in sends:
        copy.start()
    gain_copy.wait()

    def weigh(j, carry):
        own = gain_v[pl.ds(j, 1), :]
        for _, apart in chunks:
            gated_s[j, apart, :] = gated_s[j, apart, :] * own
        return carry

    lax.fori_loop(0, tiles, weigh, 0)

    for copy in sends:
        copy.wait()

    power = powers[0]
    for s in range(1, ntp):
        power = power + powers[s]
    power = power * (1.0 / (length * channels * ntp))
    inverse[...] = lax.rsqrt(power + 1e-06) * length ** (-0.5)


def emit(gated, inverse, out, inv_s, staged, sems):
    rows, channels = out.shape
    tiles = channels // LANES
    steps = rows // SUB
    pitch = spaced(steps)
    scale = inverse[...]
    for k in range(steps):
        inv_s[pl.ds(k, SUB, stride=pitch), :] = jnp.broadcast_to(scale[:, k : k + 1], (SUB, LANES))
    copies = []
    for i in range(SUB):
        dense, apart = pl.ds(i * steps, steps), pl.ds(i * pitch, steps)
        for j in range(tiles):
            staged[dense, pl.ds(j * LANES, LANES)] = (
                gated[j, apart, :] * inv_s[apart, :]
            ).astype(jnp.bfloat16)
        copies.append(pltpu.make_async_copy(staged.at[dense], out.at[dense], sems.at[i]))
        copies[-1].start()
    for copy in copies:
        copy.wait()


def body(nsp, ntp, decay_rate, drive_in, gate_in, norm_gain):
    batch, rows, channels = decay_rate.shape
    tiles = channels // LANES
    steps = rows // SUB
    width = -(-steps // LANES) * LANES
    plane = pltpu.VMEM((tiles, rows, LANES), jnp.float32)
    wide = pltpu.VMEM((tiles, SUB * spaced(steps), LANES), jnp.float32)
    half = pltpu.VMEM((tiles, rows, LANES), jnp.bfloat16)
    outside = pl.BlockSpec(memory_space=pltpu.HBM)
    vmem = pl.BlockSpec(memory_space=pltpu.VMEM)
    gated, inverse = pl.pallas_call(
        functools.partial(kernel, nsp, ntp),
        out_shape=(
            pltpu.VMEM((tiles, SUB * spaced(steps), LANES), jnp.float32),
            pltpu.VMEM((SUB, width), jnp.float32),
        ),
        in_specs=[outside] * 4,
        out_specs=(vmem, vmem),
        scratch_shapes=[
            plane, half, half, wide, wide, wide, plane, plane, plane,
            pltpu.VMEM((4, tiles, SUB, LANES), jnp.float32),
            pltpu.VMEM((nsp, 3, tiles, LANES), jnp.float32),
            pltpu.VMEM((ntp, SUB, width), jnp.float32),
            pltpu.VMEM((tiles, LANES), jnp.float32),
            pltpu.SemaphoreType.DMA,
            pltpu.SemaphoreType.DMA((3, tiles)),
            pltpu.SemaphoreType.DMA((nsp,)),
            pltpu.SemaphoreType.DMA((nsp,)),
            pltpu.SemaphoreType.DMA((ntp,)),
            pltpu.SemaphoreType.DMA((ntp,)),
        ],
        compiler_params=pltpu.CompilerParams(
            collective_id=0, has_side_effects=True, vmem_limit_bytes=52 * 1024 * 1024
        ),
    )(*(
        pltpu.with_memory_space_constraint(value, pltpu.HBM)
        for value in (
            decay_rate.reshape(rows, channels),
            drive_in.reshape(rows, channels),
            gate_in.reshape(rows, channels),
            norm_gain.reshape(tiles, LANES),
        )
    ))
    result = pl.pallas_call(
        emit,
        out_shape=jax.ShapeDtypeStruct((rows, channels), jnp.bfloat16),
        in_specs=[vmem, vmem],
        out_specs=outside,
        scratch_shapes=[
            pltpu.VMEM((SUB * spaced(steps), LANES), jnp.float32),
            pltpu.VMEM((rows, channels), jnp.bfloat16),
            pltpu.SemaphoreType.DMA((SUB,)),
        ],
        compiler_params=pltpu.CompilerParams(vmem_limit_bytes=32 * 1024 * 1024),
    )(
        pltpu.with_memory_space_constraint(gated, pltpu.VMEM),
        pltpu.with_memory_space_constraint(inverse, pltpu.VMEM),
    )
    return result.reshape(batch, rows, channels)


def solution(mesh):
    in_specs = (P(None, "sp", "tp"), P(None, "sp", "tp"), P(None, "sp", "tp"), P("tp"))
    out_specs = P(None, "sp", "tp")
    local = functools.partial(body, mesh.shape["sp"], mesh.shape["tp"])
    return jax.shard_map(local, mesh=mesh, in_specs=in_specs, out_specs=out_specs, check_vma=False)
```
